32 devices in a mesh: row: 16 (over z, y, x), col: 2 (over core).
Axes of the slice: x: 2, y: 2, z: 4, core: 2. Of those that a mesh axis runs over, the one named last changes fastest.
Arguments:
- right_sides: bfloat16 [256, 128, 128], P('row'), may hold values from -6 to 6
- inverse_diag: bfloat16 [256, 128, 128], P('row'), may hold values from -0.5 to 0.5
- off_blocks: bfloat16 [2, 256, 6, 128, 128], P('col', 'row'), may hold values from -0.09375 to 0.09375
- owners: int32 [2, 256, 6], P('col', 'row'), may hold values from 0 to 15, all different within a row; in each aligned block of 16 rows (0 to 15, 16 to 31, ..., all dimensions but the last counted through in order) at most 8 rows name the same one
- local_block: int32 [2, 256, 6], P('col', 'row'), may hold values from 0 to 15
- counts: int32 [256], P('row'), may hold values from 6 to 12
Outputs:
- solved: bfloat16 [256, 128, 128], P('row')
The draws below stay inside these ranges and needn't reach their ends.
Inputs may be any that keep to these rules, and one draw needn't show every extreme that they name: In the 16 block rows of one device (aligned blocks of rows of the [2, 256] layout) a row's 6 entries are different owners, no owner is named more than 8 times, and in some blocks one owner exactly 8 times.
All inputs are finite; a program needn't handle non-finite values.
Results may differ from the reference program's by a relative error of at most 0.014.
Values may be sent and summed in bfloat16 or wider, within the bound.
A program may use at most 64 MiB of HBM per device.

```python
import math
import jax
import jax.numpy as jnp
import numpy as np
from jax import lax

BLOCK = 128
RHS = 128
BR_DEV = 16
KD = 6
ITERS = 4
NB = 256
KSLOTS = 12
CAP = 8
N_ROW = 16
N_COL = 2


def set_ends(values, stream_key, smallest, top_value):
    extent = values.shape
    index_at = [jax.random.randint(jax.random.fold_in(stream_key, axis), (), 0, extent[axis]) for axis in range(len(extent))]
    values = values.at[tuple(index_at)].set(smallest)
    longest = extent.index(max(extent))
    index_at[longest] = (index_at[longest] + 1) % extent[longest]
    return values.at[tuple(index_at)].set(top_value)


def level_of(rng, dims, cuts, low, high):
    def one(position, shards_of):
        heights = jax.random.uniform(jax.random.fold_in(jax.random.fold_in(rng, 6), position), (shards_of,), jnp.float32, low / len(cuts), high / len(cuts))
        return jnp.repeat(jnp.exp(heights), dims[position] // shards_of).reshape((-1,) + (1,) * (len(dims) - position - 1))

    gain = one(*cuts[0])
    for cut in cuts[1:]:
        gain = gain * one(*cut)
    return gain


def routed_block(key, own, number, rows, count, top, limit, skew):
    ranking = jax.random.permutation(key, count)
    heavy_load, ordinary = load_shares(count, rows * top, limit, skew, True), load_shares(count, rows * top, limit, skew, False)
    places = jnp.arange(count)

    def named(lengths, turn):
        used = int((lengths > 0).sum())
        fixed = max(1, used // 4)
        passed = fixed + (places - fixed + turn * (used - fixed)) % max(1, count - fixed)
        return jnp.zeros((count,), jnp.int32).at[ranking[jnp.where(places < fixed, places, passed)]].set(jnp.asarray(lengths, jnp.int32))

    lengths = jnp.where(number % 4 == 0, named(heavy_load, number // 4), named(ordinary, number - number // 4 - 1))
    mixed = jax.random.permutation(jax.random.fold_in(own, 3), count)
    source_of, sink = mixed[0:count // 2 * 2:2], mixed[1:count // 2 * 2:2]
    margin = jnp.minimum(lengths[source_of] - 1, limit - lengths[sink]) // 2
    margin = jnp.where((source_of == ranking[0]) | (sink == ranking[0]) | (lengths[sink] == 0), 0, jnp.maximum(margin, 0))
    passed = jax.random.randint(jax.random.fold_in(own, 4), (count // 2,), 0, 1 << 20) % (margin + 1)
    lengths = lengths.at[source_of].add(-passed).at[sink].add(passed)
    labels = jnp.searchsorted(jnp.cumsum(lengths), jnp.arange(rows * top), side="right").astype(jnp.int32)
    table = labels.reshape(top, rows).T
    table = table[jax.random.permutation(jax.random.fold_in(own, 1), rows)]
    turn = jax.random.randint(jax.random.fold_in(own, 2), (rows, 1), 0, top)
    return jnp.take_along_axis(table, (jnp.arange(top)[None, :] + turn) % top, axis=1)


def load_shares(count, total, most, lean, full):
    loads = [(1 << 20) // math.isqrt(rank ** lean) + 1 for rank in range(1, count + 1)]
    largest = most if full else min(most, max(-(-total // count), total * loads[0] // sum(loads)))
    least = 1 if total - largest >= count - 1 else 0
    given, rest = [largest] + [least] * (count - 1), total - largest - least * (count - 1)
    while rest > 0:
        free = [i for i in range(1, count) if given[i] < largest] or [i for i in range(1, count) if given[i] < most]
        whole, left = sum([loads[i] for i in free]), rest
        for i in free:
            extra = min(most - given[i], max(1, left * loads[i] // whole), rest)
            given[i] = given[i] + extra
            rest = rest - extra
    return np.array(given)


def centred(key, dims, deviation, reach, shards=(), held_as=jnp.bfloat16):
    values = jax.random.normal(key, dims, jnp.float32) * deviation
    if len(shards) > 0:
        values = level_of(key, dims, shards, -0.22, 0.18) * values
    return jnp.clip(values, min=-reach, max=reach).astype(held_as)


def setup_inputs(seed: int = 0) -> dict:
    streams_of = jax.random.split(jax.random.key(seed), 7)
    right_sides = centred(streams_of[0], (NB, BLOCK, RHS), 1.0, 6.0, ((0, 16),))
    inverse_diag = centred(streams_of[1], (NB, BLOCK, BLOCK), BLOCK ** -0.5, 0.5, ((0, 16),))
    off_blocks = centred(streams_of[2], (N_COL, NB, KD, BLOCK, BLOCK), (3 * BLOCK * KSLOTS) ** -0.5, 0.09375, ((0, 2), (1, 16)))
    owners_keys = jax.random.split(jax.random.fold_in(streams_of[3], 1), N_COL * NB // BR_DEV)
    owners_turns = jax.random.permutation(jax.random.fold_in(streams_of[3], 3), N_COL * NB // BR_DEV)
    owners = jax.vmap(lambda own, number: routed_block(jax.random.fold_in(streams_of[3], 2), own, number, BR_DEV, N_ROW, KD, CAP, 2))(owners_keys, owners_turns).reshape((N_COL, NB, KD))
    local_block = set_ends(jax.random.randint(streams_of[4], (N_COL, NB, KD), 0, BR_DEV), jax.random.fold_in(streams_of[4], 1), 0, BR_DEV - 1).astype(jnp.int32)
    counts = set_ends(jax.random.randint(streams_of[5], (NB,), KSLOTS // 2, KSLOTS + 1), jax.random.fold_in(streams_of[5], 1), KSLOTS // 2, KSLOTS).astype(jnp.int32)
    return {"right_sides": right_sides, "inverse_diag": inverse_diag, "off_blocks": off_blocks, "owners": owners, "local_block": local_block, "counts": counts}


def apply_inverse(inverse, right):
    return jnp.einsum("bij,bjr->bir", inverse.astype(jnp.float32), right.astype(jnp.float32)).astype(jnp.bfloat16)


def reference(right_sides, inverse_diag, off_blocks, owners, local_block, counts):
    group_count = owners.shape[0]
    per_group = owners.shape[2]
    columns = (owners * BR_DEV + local_block).astype(jnp.int32)
    slot_index = jnp.arange(group_count, dtype=jnp.int32)[:, None, None] + group_count * jnp.arange(per_group, dtype=jnp.int32)[None, None, :]
    is_live = slot_index < counts[None, :, None]
    solved = apply_inverse(inverse_diag, right_sides)
    for iteration in range(ITERS - 1):
        current = solved

        def group_term(pieces):
            blocks, cols, live = pieces
            picked = current[cols].astype(jnp.float32)
            masked = jnp.where(live[:, :, None, None], blocks.astype(jnp.float32), jnp.zeros((), jnp.float32))
            return jnp.einsum("bkij,bkjr->bir", masked, picked).astype(jnp.bfloat16)

        partial_value = lax.map(group_term, (off_blocks, columns, is_live))
        off_sum = jnp.sum(partial_value.astype(jnp.float32), axis=0)
        corrected = (right_sides.astype(jnp.float32) - off_sum).astype(jnp.bfloat16)
        solved = apply_inverse(inverse_diag, corrected)
    return solved
```

```python
import functools

import jax
import jax.numpy as jnp
from jax import lax
from jax.experimental import pallas as pl
from jax.experimental.pallas import tpu as pltpu
from jax.sharding import PartitionSpec as P

ITERS = 4
MESH = pl.DeviceIdType.MESH
PIECES = ("zxy", "zyx", "xyz", "yxz")
EIGHTHS = (3, 3, 1, 1)
TO_X, TO_Y, TO_UP, TO_DOWN, TO_COL = range(5)


def kernel(
    n_row,
    n_col,
    columns,
    rhs_hbm,
    inv_hbm,
    off_hbm,
    out,
    xg,
    off,
    rhs,
    inv,
    mine,
    outgoing,
    incoming,
    load_sem,
    recv_sem,
    send_sem,
    col_sem,
    part_send,
    part_recv,
    out_send,
    out_recv,
    ready,
):
    row, col = lax.axis_index("row"), lax.axis_index("col")
    block_rows, per_group, size = off.shape[0], off.shape[1], off.shape[2]
    share = block_rows // n_col
    by_blocks = share % 8 == 0
    n_z = n_row // 4
    x, y, z = row % 2, (row // 2) % 2, row // 4
    has_up, has_down = z < n_z - 1, z > 0
    target_row = {
        TO_X: row + 1 - 2 * x,
        TO_Y: row + 2 - 4 * y,
        TO_UP: row + 4,
        TO_DOWN: row - 4,
    }
    back = {TO_X: TO_X, TO_Y: TO_Y, TO_UP: TO_DOWN, TO_DOWN: TO_UP}
    others = [(col + step) % n_col for step in range(1, n_col)]

    loads = []
    first = col * share
    for number, (src, dst) in enumerate(
        (
            (rhs_hbm.at[pl.ds(first, share)], rhs),
            (inv_hbm.at[pl.ds(first, share)], inv),
            (off_hbm, off),
        )
    ):
        copy = pltpu.make_async_copy(src, dst, load_sem.at[number])
        copy.start()
        loads.append(copy)

    def greet(semaphore_of):
        for to in (TO_X, TO_Y):
            pl.semaphore_signal(
                semaphore_of(back[to]), inc=1, device_id=(target_row[to], col), device_id_type=MESH
            )
        for to, there in ((TO_UP, has_up), (TO_DOWN, has_down)):

            @pl.when(there)
            def _():
                pl.semaphore_signal(
                    semaphore_of(back[to]),
                    inc=1,
                    device_id=(target_row[to], col),
                    device_id_type=MESH,
                )

        for step, other in enumerate(others):
            pl.semaphore_signal(
                semaphore_of(TO_COL + step), inc=1, device_id=(row, other), device_id_type=MESH
            )

    barrier = pltpu.get_barrier_semaphore()
    greet(lambda which: barrier)
    pl.semaphore_wait(
        barrier, 2 + len(others) + has_up.astype(jnp.int32) + has_down.astype(jnp.int32)
    )

    def start_of(of_col, of_row):
        return (of_col * n_row + of_row) * share

    def whole_share(of_col, of_row):
        return xg.at[pl.ds(start_of(of_col, of_row), share)]

    def piece_of(piece, src):
        begin, eighths = sum(EIGHTHS[:piece]), EIGHTHS[piece]
        if by_blocks:
            return xg.at[pl.ds(start_of(col, src) + begin * share // 8, eighths * share // 8)]
        rows = size // 8
        return xg.at[pl.ds(start_of(col, src), share), pl.ds(begin * rows, eighths * rows)]

    def eighths_of_share(eighths):
        if by_blocks:
            return xg.at[pl.ds(0, eighths * share // 8)]
        return xg.at[pl.ds(0, eighths * share), pl.ds(0, size // 8)]

    def remote(piece, src, to):
        return pltpu.make_async_remote_copy(
            src_ref=piece_of(piece, src),
            dst_ref=piece_of(piece, src),
            send_sem=send_sem.at[to],
            recv_sem=recv_sem.at[piece, src],
            device_id=(target_row[to], col),
            device_id_type=MESH,
        )

    def send(piece, src, to):
        remote(piece, src, to).start()

    def arrived(piece, src):
        remote(piece, src, TO_X).wait_recv()

    def send_z(piece, src, ways=(TO_UP, TO_DOWN)):
        for to in ways:

            @pl.when(has_up if to == TO_UP else has_down)
            def _():
                send(piece, src, to)

    def share_copy(src, step):
        return pltpu.make_async_remote_copy(
            src_ref=whole_share(col, src),
            dst_ref=whole_share(col, src),
            send_sem=send_sem.at[TO_COL + step],
            recv_sem=col_sem.at[step, src],
            device_id=(row, others[step]),
            device_id_type=MESH,
        )

    def at(plane, flip_y, flip_x):
        there_y = 1 - y if flip_y else y
        there_x = 1 - x if flip_x else x
        return plane * 4 + there_y * 2 + there_x

    FLIPS = ((0, 0), (0, 1), (1, 0), (1, 1))

    def spread_plane(plane):
        arrived(0, at(plane, 0, 1))
        send(0, at(plane, 0, 1), TO_Y)
        arrived(1, at(plane, 1, 0))
        send(1, at(plane, 1, 0), TO_X)
        arrived(0, at(plane, 1, 0))
        arrived(1, at(plane, 0, 1))
        arrived(0, at(plane, 1, 1))
        arrived(1, at(plane, 1, 1))

    def to_columns(plane, own):
        for flip in FLIPS:
            if own and flip == (0, 0):
                continue
            for step in range(n_col - 1):
                share_copy(at(plane, *flip), step).start()

    def gather():
        send(2, row, TO_X)
        send(3, row, TO_Y)
        send(3, row, TO_X)
        send(2, row, TO_Y)
        for piece in range(4):
            send_z(piece, row)
        send(1, row, TO_X)
        send(0, row, TO_Y)
        send(0, row, TO_X)
        send(1, row, TO_Y)
        for step in range(n_col - 1):
            share_copy(row, step).start()
        arrived(2, at(z, 0, 1))
        send(2, at(z, 0, 1), TO_Y)
        send_z(2, at(z, 0, 1))
        arrived(3, at(z, 1, 0))
        send(3, at(z, 1, 0), TO_X)
        send_z(3, at(z, 1, 0))
        for piece, flips in ((2, ((1, 0), (1, 1))), (3, ((0, 1), (1, 1)))):
            for flip in flips:
                arrived(piece, at(z, *flip))
                send_z(piece, at(z, *flip))

        for distance in range(1, n_z + 1):
            for sign, onward in ((-1, TO_UP), (1, TO_DOWN)):
                plane = z + sign * distance
                there = plane >= 0 if sign < 0 else plane < n_z

                if distance < n_z:

                    @pl.when(there)
                    def _():
                        for piece in (0, 1):
                            src = at(plane, 0, 0)
                            arrived(piece, src)
                            send_z(piece, src, (onward,))
                            for to in (TO_X, TO_Y) if piece == 1 else (TO_Y, TO_X):
                                send(piece, src, to)
                        for piece in (2, 3):
                            for flip in FLIPS:
                                arrived(piece, at(plane, *flip))
                                send_z(piece, at(plane, *flip), (onward,))

                if distance == 1:
                    if sign < 0:
                        spread_plane(z)
                        to_columns(z, True)
                    continue
                before = z + sign * (distance - 1)
                was_there = before >= 0 if sign < 0 else before < n_z

                @pl.when(was_there)
                def _():
                    spread_plane(before)
                    to_columns(before, False)

        for step in range(n_col - 1):
            sender = others[n_col - 2 - step]
            for src in range(n_row):
                pltpu.make_async_remote_copy(
                    src_ref=whole_share(sender, src),
                    dst_ref=whole_share(sender, src),
                    send_sem=send_sem.at[TO_COL + step],
                    recv_sem=col_sem.at[step, src],
                    device_id=(row, others[step]),
                    device_id_type=MESH,
                ).wait_recv()

    def sent(to, eighths):
        part = eighths_of_share(eighths)
        pltpu.make_async_copy(part, part, send_sem.at[to]).wait()

    def finish_sends():
        for to in (TO_X, TO_Y):
            sent(to, n_z * 9 + 3)
        for to, there, ahead in ((TO_UP, has_up, z), (TO_DOWN, has_down, n_z - 1 - z)):
            for earlier in range(n_z - 1):

                @pl.when(jnp.logical_and(there, earlier <= ahead))
                def _():
                    sent(to, 14)

        for step in range(n_col - 1):
            sent(TO_COL + step, 8 * n_row)

    def product(i):
        left = jnp.concatenate([off[i, k] for k in range(per_group)], axis=1)
        right = jnp.concatenate(
            [xg[columns[i * per_group + k]] for k in range(per_group)], axis=0
        )
        return jnp.dot(left, right, preferred_element_type=jnp.float32).astype(jnp.bfloat16)

    def part_copy(step):
        return pltpu.make_async_remote_copy(
            src_ref=outgoing.at[step],
            dst_ref=incoming.at[step],
            send_sem=part_send.at[step],
            recv_sem=part_recv.at[step],
            device_id=(row, others[step]),
            device_id_type=MESH,
        )

    own_start = start_of(col, row)

    xg[n_col * n_row * share] = jnp.zeros(xg.shape[1:], xg.dtype)
    loads[0].wait()
    loads[1].wait()

    for j in range(share):
        solved = jnp.dot(inv[j], rhs[j], preferred_element_type=jnp.float32)
        xg[own_start + j] = solved.astype(jnp.bfloat16)
    loads[2].wait()

    def iterate(turn, carry):
        @pl.when(turn > 0)
        def _():
            for to in (TO_X, TO_Y):
                pl.semaphore_wait(ready.at[to], 1)
            for to, there in ((TO_UP, has_up), (TO_DOWN, has_down)):

                @pl.when(there)
                def _():
                    pl.semaphore_wait(ready.at[to], 1)

            for step in range(n_col - 1):
                pl.semaphore_wait(ready.at[TO_COL + step], 1)

        gather()
        finish_sends()
        for step in range(n_col - 1):
            for j in range(share):
                outgoing[step, j] = product(others[step] * share + j)
            part_copy(step).start()
        for j in range(share):
            mine[j] = product(col * share + j).astype(jnp.float32)

        @pl.when(turn < ITERS - 2)
        def _():
            greet(lambda which: ready.at[which])

        for step in range(n_col - 1):
            part_copy(step).wait()
        for j in range(share):
            total = mine[j]
            for step in range(n_col - 1):
                total = total + incoming[step, j].astype(jnp.float32)
            corrected = (rhs[j].astype(jnp.float32) - total).astype(jnp.bfloat16)
            solved = jnp.dot(inv[j], corrected, preferred_element_type=jnp.float32)
            xg[own_start + j] = solved.astype(jnp.bfloat16)
        return carry

    lax.fori_loop(0, ITERS - 1, iterate, 0)

    def out_copy(step):
        part = out.at[pl.ds(col * share, share)]
        return pltpu.make_async_remote_copy(
            src_ref=whole_share(col, row),
            dst_ref=part,
            send_sem=out_send.at[step],
            recv_sem=out_recv.at[step],
            device_id=(row, others[step]),
            device_id_type=MESH,
        )

    for step in range(n_col - 1):
        out_copy(step).start()
    out[pl.ds(col * share, share)] = xg[pl.ds(own_start, share)]
    for step in range(n_col - 1):
        out_copy(step).wait()


def shards(n_row, n_col, right_sides, inverse_diag, off_blocks, owners, local_block, counts):
    block_rows, size, width = right_sides.shape
    per_group = owners.shape[2]
    share = block_rows // n_col
    slot = lax.axis_index("col") + n_col * jnp.arange(per_group, dtype=jnp.int32)
    place = local_block[0]
    found = (place // share) * (n_row * share) + owners[0] * share + place % share
    columns = jnp.where(slot[None, :] < counts[:, None], found, n_row * block_rows).reshape(-1)
    smem = pl.BlockSpec(memory_space=pltpu.SMEM)
    hbm = pl.BlockSpec(memory_space=pl.ANY)
    bf16 = jnp.bfloat16
    dma = pltpu.SemaphoreType.DMA
    return pl.pallas_call(
        functools.partial(kernel, n_row, n_col),
        out_shape=jax.ShapeDtypeStruct(right_sides.shape, bf16),
        in_specs=[smem, hbm, hbm, hbm],
        out_specs=pl.BlockSpec(memory_space=pltpu.VMEM),
        scratch_shapes=[
            pltpu.VMEM((n_row * block_rows + 1, size, width), bf16),
            pltpu.VMEM((block_rows, per_group, size, size), bf16),
            pltpu.VMEM((share, size, width), bf16),
            pltpu.VMEM((share, size, size), bf16),
            pltpu.VMEM((share, size, width), jnp.float32),
            pltpu.VMEM((n_col - 1, share, size, width), bf16),
            pltpu.VMEM((n_col - 1, share, size, width), bf16),
            dma((3,)),
            dma((4, n_row)),
            dma((4 + n_col - 1,)),
            dma((n_col - 1, n_row)),
            dma((n_col - 1,)),
            dma((n_col - 1,)),
            dma((n_col - 1,)),
            dma((n_col - 1,)),
            pltpu.SemaphoreType.REGULAR((4 + n_col - 1,)),
        ],
        compiler_params=pltpu.CompilerParams(
            collective_id=0, has_side_effects=True, vmem_limit_bytes=60 * 1024 * 1024
        ),
    )(
        columns,
        right_sides,
        inverse_diag,
        off_blocks.reshape(off_blocks.shape[1:]),
    )


def solution(mesh):
    in_specs = (
        P("row", None, None),
        P("row", None, None),
        P("col", "row", None, None, None),
        P("col", "row", None),
        P("col", "row", None),
        P("row"),
    )
    body = functools.partial(shards, mesh.shape["row"], mesh.shape["col"])
    return jax.shard_map(
        body, mesh=mesh, in_specs=in_specs, out_specs=P("row", None, None), check_vma=False
    )
```

```python
import functools
import heapq

import jax
import jax.numpy as jnp
from jax import lax
from jax.experimental import pallas as pl
from jax.experimental.pallas import tpu as pltpu
from jax.sharding import PartitionSpec as P

ITERS = 4
MESH = pl.DeviceIdType.MESH
TO_X, TO_Y, TO_UP, TO_DOWN, TO_COL = range(5)
FOUR = (3, 3, 1, 1)
EIGHT = (1,) * 8
EDGE = ("zxy", "zyx", "zxy", "xzy", "yxz", "yzx", "zyx", "xzy")
INNER = ("zyx", "zxy", "zyx", "yzx", "xzy", "zxy", "zyx", "yxz")
ORDERS = ("zxy", "zyx", "xyz", "yxz", "xzy", "yzx")
DEPTH_WEIGHT, DISTANCE_WEIGHT = 0.73, 0.08
PLANE_WEIGHT = dict(zip(ORDERS, (0.62, -0.3, -0.43, -0.82, 0.14, 0.07)))
LINE_WEIGHT = dict(zip(ORDERS, (-1.84, -0.38, 0.41, -1.4, -1.52, -2.03)))
PIECE_TIME, LATENCY, AHEAD = 0.703, 1.6, 1.5


def targets(order, n_z, z, src_z, flip_y, flip_x):
    moved = {"x": flip_x, "y": flip_y, "z": src_z != z}
    found = []
    for place, axis in enumerate(order):
        if any(moved[later] for later in order[place + 1 :]):
            continue
        if axis == "z":
            if src_z <= z < n_z - 1:
                found.append(TO_UP)
            if src_z >= z > 0:
                found.append(TO_DOWN)
        elif not moved[axis]:
            found.append(TO_X if axis == "x" else TO_Y)
    return found


def beyond(z, src_z, flip_y, flip_x, to):
    return {
        TO_X: (z, src_z, flip_y, 1 - flip_x),
        TO_Y: (z, src_z, 1 - flip_y, flip_x),
        TO_UP: (z + 1, src_z, flip_y, flip_x),
        TO_DOWN: (z - 1, src_z, flip_y, flip_x),
    }[to]


@functools.lru_cache(None)
def depth(order, n_z, *where):
    ways = targets(order, n_z, *where)
    return max((1 + depth(order, n_z, *beyond(*where, to)) for to in ways), default=0)


def planned(n_z):
    orders = [EDGE if z in (0, n_z - 1) else INNER for z in range(n_z)]
    events, queued, busy = [], {}, {}
    log = [[] for _ in range(n_z)]
    count = 0
    for z in range(n_z):
        for piece in range(len(EIGHT)):
            events.append((0.0, count, None, piece, (z, z, 0, 0)))
            count += 1
    heapq.heapify(events)
    while events:
        now, touched = events[0][0], set()
        while events and events[0][0] <= now + 1e-9:
            _, _, link, piece, where = heapq.heappop(events)
            if link is not None:
                busy[link] = False
                touched.add(link)
                continue
            z, src_z, flip_y, flip_x = where
            if where != (z, z, 0, 0):
                log[z].append((now, 0, count, (piece, src_z, flip_y, flip_x)))
            order = orders[src_z][piece]
            for to in targets(order, n_z, *where):
                weight = PLANE_WEIGHT if to in (TO_X, TO_Y) else LINE_WEIGHT
                rank = (
                    weight[order]
                    + DISTANCE_WEIGHT * abs(src_z - z)
                    - DEPTH_WEIGHT * depth(order, n_z, *beyond(*where, to))
                )
                heapq.heappush(queued.setdefault((z, to), []), (rank, now, count, piece, where))
                touched.add((z, to))
                count += 1
        for link in sorted(touched):
            if busy.get(link) or not queued.get(link):
                continue
            _, known, _, piece, where = heapq.heappop(queued[link])
            z, to = link
            busy[link] = True
            log[z].append((max(known, now - AHEAD), 1, count, (piece, *where[1:], to)))
            heapq.heappush(events, (now + PIECE_TIME, count + 1, link, None, None))
            heapq.heappush(
                events, (now + PIECE_TIME + LATENCY, count + 2, None, piece, beyond(*where, to))
            )
            count += 3
    return [[entry[3] for entry in sorted(one)] for one in log]


def kernel(
    n_row,
    n_col,
    columns,
    rhs_hbm,
    inv_hbm,
    off_hbm,
    out,
    xg,
    off,
    rhs,
    inv,
    mine,
    outgoing,
    incoming,
    load_sem,
    recv_sem,
    send_sem,
    col_sem,
    part_send,
    part_recv,
    out_send,
    out_recv,
    ready,
):
    row, col = lax.axis_index("row"), lax.axis_index("col")
    block_rows, per_group, size = off.shape[0], off.shape[1], off.shape[2]
    share = block_rows // n_col
    by_blocks = share % 8 == 0
    short = n_row // 4 <= 4
    eighths_of = EIGHT if short else FOUR
    n_z = n_row // 4
    x, y, z = row % 2, (row // 2) % 2, row // 4
    has_up, has_down = z < n_z - 1, z > 0
    target_row = {
        TO_X: row + 1 - 2 * x,
        TO_Y: row + 2 - 4 * y,
        TO_UP: row + 4,
        TO_DOWN: row - 4,
    }
    back = {TO_X: TO_X, TO_Y: TO_Y, TO_UP: TO_DOWN, TO_DOWN: TO_UP}
    others = [(col + step) % n_col for step in range(1, n_col)]

    loads = []
    first = col * share
    for number, (src, dst) in enumerate(
        (
            (rhs_hbm.at[pl.ds(first, share)], rhs),
            (inv_hbm.at[pl.ds(first, share)], inv),
            (off_hbm, off),
        )
    ):
        copy = pltpu.make_async_copy(src, dst, load_sem.at[number])
        copy.start()
        loads.append(copy)

    def greet(semaphore_of):
        for to in (TO_X, TO_Y):
            pl.semaphore_signal(
                semaphore_of(back[to]), inc=1, device_id=(target_row[to], col), device_id_type=MESH
            )
        for to, there in ((TO_UP, has_up), (TO_DOWN, has_down)):

            @pl.when(there)
            def _():
                pl.semaphore_signal(
                    semaphore_of(back[to]),
                    inc=1,
                    device_id=(target_row[to], col),
                    device_id_type=MESH,
                )

        for step, other in enumerate(others):
            pl.semaphore_signal(
                semaphore_of(TO_COL + step), inc=1, device_id=(row, other), device_id_type=MESH
            )

    barrier = pltpu.get_barrier_semaphore()
    greet(lambda which: barrier)
    pl.semaphore_wait(
        barrier, 2 + len(others) + has_up.astype(jnp.int32) + has_down.astype(jnp.int32)
    )

    def start_of(of_col, of_row):
        return of_row * block_rows + of_col * share

    def whole_share(of_col, of_row):
        return xg.at[pl.ds(start_of(of_col, of_row), share)]

    def piece_of(piece, src):
        return part_of(src, sum(eighths_of[:piece]), eighths_of[piece])

    def part_of(src, begin, eighths):
        if by_blocks:
            return xg.at[pl.ds(start_of(col, src) + begin * share // 8, eighths * share // 8)]
        rows = size // 8
        return xg.at[pl.ds(start_of(col, src), share), pl.ds(begin * rows, eighths * rows)]

    def eighths_of_share(eighths):
        if by_blocks:
            return xg.at[pl.ds(0, eighths * share // 8)]
        return xg.at[pl.ds(0, eighths * share), pl.ds(0, size // 8)]

    def remote(piece, src, to):
        return pltpu.make_async_remote_copy(
            src_ref=piece_of(piece, src),
            dst_ref=piece_of(piece, src),
            send_sem=send_sem.at[to],
            recv_sem=recv_sem.at[piece, src],
            device_id=(target_row[to], col),
            device_id_type=MESH,
        )

    def send(piece, src, to):
        remote(piece, src, to).start()

    def arrived(piece, src):
        remote(piece, src, TO_X).wait_recv()

    def send_z(piece, src, ways=(TO_UP, TO_DOWN)):
        for to in ways:

            @pl.when(has_up if to == TO_UP else has_down)
            def _():
                send(piece, src, to)

    def share_copy(src, step, begin=0, eighths=8):
        return pltpu.make_async_remote_copy(
            src_ref=part_of(src, begin, eighths),
            dst_ref=part_of(src, begin, eighths),
            send_sem=send_sem.at[TO_COL + step],
            recv_sem=col_sem.at[step, src],
            device_id=(row, others[step]),
            device_id_type=MESH,
        )

    def at(plane, flip_y, flip_x):
        there_y = 1 - y if flip_y else y
        there_x = 1 - x if flip_x else x
        return plane * 4 + there_y * 2 + there_x

    FLIPS = ((0, 0), (0, 1), (1, 0), (1, 1))

    def spread_plane(plane):
        arrived(0, at(plane, 0, 1))
        send(0, at(plane, 0, 1), TO_Y)
        arrived(1, at(plane, 1, 0))
        send(1, at(plane, 1, 0), TO_X)
        arrived(0, at(plane, 1, 0))
        arrived(1, at(plane, 0, 1))
        arrived(0, at(plane, 1, 1))
        arrived(1, at(plane, 1, 1))

    def to_columns(plane, own):
        for flip in FLIPS:
            if own and flip == (0, 0):
                continue
            for step in range(n_col - 1):
                share_copy(at(plane, *flip), step).start()

    def gather():
        send(2, row, TO_X)
        send(3, row, TO_Y)
        send(3, row, TO_X)
        send(2, row, TO_Y)
        for piece in range(4):
            send_z(piece, row)
        send(1, row, TO_X)
        send(0, row, TO_Y)
        send(0, row, TO_X)
        send(1, row, TO_Y)
        for step in range(n_col - 1):
            share_copy(row, step).start()
        arrived(2, at(z, 0, 1))
        send(2, at(z, 0, 1), TO_Y)
        send_z(2, at(z, 0, 1))
        arrived(3, at(z, 1, 0))
        send(3, at(z, 1, 0), TO_X)
        send_z(3, at(z, 1, 0))
        for piece, flips in ((2, ((1, 0), (1, 1))), (3, ((0, 1), (1, 1)))):
            for flip in flips:
                arrived(piece, at(z, *flip))
                send_z(piece, at(z, *flip))

        for distance in range(1, n_z + 1):
            for sign, onward in ((-1, TO_UP), (1, TO_DOWN)):
                plane = z + sign * distance
                there = plane >= 0 if sign < 0 else plane < n_z

                if distance < n_z:

                    @pl.when(there)
                    def _():
                        for piece in (0, 1):
                            src = at(plane, 0, 0)
                            arrived(piece, src)
                            send_z(piece, src, (onward,))
                            for to in (TO_X, TO_Y) if piece == 1 else (TO_Y, TO_X):
                                send(piece, src, to)
                        for piece in (2, 3):
                            for flip in FLIPS:
                                arrived(piece, at(plane, *flip))
                                send_z(piece, at(plane, *flip), (onward,))

                if distance == 1:
                    if sign < 0:
                        spread_plane(z)
                        to_columns(z, True)
                    continue
                before = z + sign * (distance - 1)
                was_there = before >= 0 if sign < 0 else before < n_z

                @pl.when(was_there)
                def _():
                    spread_plane(before)
                    to_columns(before, False)

    def gather_by_plan(my_z, plan):
        have = {}
        sent_to = dict.fromkeys((TO_X, TO_Y, TO_UP, TO_DOWN), 0)
        for step in range(n_col - 1):
            share_copy(row, step).start()
        for piece, src_z, flip_y, flip_x, *to in plan:
            src = at(src_z, flip_y, flip_x)
            if to:
                send(piece, src, to[0])
                sent_to[to[0]] += 1
                continue
            arrived(piece, src)
            half = (src_z, flip_y, flip_x, piece // 4)
            have[half] = have.get(half, 0) + 1
            if have[half] == 4:
                for step in range(n_col - 1):
                    share_copy(src, step, piece // 4 * 4, 4).start()
        for to, number in sent_to.items():
            if number:
                sent(to, number)

    def finish_columns():
        for step in range(n_col - 1):
            sender = others[n_col - 2 - step]
            for src in range(n_row):
                pltpu.make_async_remote_copy(
                    src_ref=whole_share(sender, src),
                    dst_ref=whole_share(sender, src),
                    send_sem=send_sem.at[TO_COL + step],
                    recv_sem=col_sem.at[step, src],
                    device_id=(row, others[step]),
                    device_id_type=MESH,
                ).wait_recv()
            sent(TO_COL + step, 8 * n_row)

    def sent(to, eighths):
        part = eighths_of_share(eighths)
        pltpu.make_async_copy(part, part, send_sem.at[to]).wait()

    def finish_sends():
        for to in (TO_X, TO_Y):
            sent(to, n_z * 9 + 3)
        for to, there, ahead in ((TO_UP, has_up, z), (TO_DOWN, has_down, n_z - 1 - z)):
            for earlier in range(n_z - 1):

                @pl.when(jnp.logical_and(there, earlier <= ahead))
                def _():
                    sent(to, 14)


    def product(i):
        left = jnp.concatenate([off[i, k] for k in range(per_group)], axis=1)
        right = jnp.concatenate(
            [xg[columns[i * per_group + k]] for k in range(per_group)], axis=0
        )
        return jnp.dot(left, right, preferred_element_type=jnp.float32).astype(jnp.bfloat16)

    def part_copy(step):
        return pltpu.make_async_remote_copy(
            src_ref=outgoing.at[step],
            dst_ref=incoming.at[step],
            send_sem=part_send.at[step],
            recv_sem=part_recv.at[step],
            device_id=(row, others[step]),
            device_id_type=MESH,
        )

    own_start = start_of(col, row)

    xg[n_col * n_row * share] = jnp.zeros(xg.shape[1:], xg.dtype)
    loads[0].wait()
    loads[1].wait()

    for j in range(share):
        solved = jnp.dot(inv[j], rhs[j], preferred_element_type=jnp.float32)
        xg[own_start + j] = solved.astype(jnp.bfloat16)
    loads[2].wait()

    def iterate(turn, carry):
        @pl.when(turn > 0)
        def _():
            for to in (TO_X, TO_Y):
                pl.semaphore_wait(ready.at[to], 1)
            for to, there in ((TO_UP, has_up), (TO_DOWN, has_down)):

                @pl.when(there)
                def _():
                    pl.semaphore_wait(ready.at[to], 1)

            for step in range(n_col - 1):
                pl.semaphore_wait(ready.at[TO_COL + step], 1)

        if short:
            for my_z, plan in enumerate(planned(n_z)):
                pl.when(z == my_z)(functools.partial(gather_by_plan, my_z, plan))
        else:
            gather()
            finish_sends()
        finish_columns()
        for step in range(n_col - 1):
            for j in range(share):
                outgoing[step, j] = product(others[step] * share + j)
            part_copy(step).start()
        for j in range(share):
            mine[j] = product(col * share + j).astype(jnp.float32)

        @pl.when(turn < ITERS - 2)
        def _():
            greet(lambda which: ready.at[which])

        for step in range(n_col - 1):
            part_copy(step).wait()
        for j in range(share):
            total = mine[j]
            for step in range(n_col - 1):
                total = total + incoming[step, j].astype(jnp.float32)
            corrected = (rhs[j].astype(jnp.float32) - total).astype(jnp.bfloat16)
            solved = jnp.dot(inv[j], corrected, preferred_element_type=jnp.float32)
            xg[own_start + j] = solved.astype(jnp.bfloat16)
        return carry

    lax.fori_loop(0, ITERS - 1, iterate, 0)

    def out_copy(step):
        part = out.at[pl.ds(col * share, share)]
        return pltpu.make_async_remote_copy(
            src_ref=whole_share(col, row),
            dst_ref=part,
            send_sem=out_send.at[step],
            recv_sem=out_recv.at[step],
            device_id=(row, others[step]),
            device_id_type=MESH,
        )

    for step in range(n_col - 1):
        out_copy(step).start()
    out[pl.ds(col * share, share)] = xg[pl.ds(own_start, share)]
    for step in range(n_col - 1):
        out_copy(step).wait()


def shards(n_row, n_col, right_sides, inverse_diag, off_blocks, owners, local_block, counts):
    block_rows, size, width = right_sides.shape
    per_group = owners.shape[2]
    share = block_rows // n_col
    slot = lax.axis_index("col") + n_col * jnp.arange(per_group, dtype=jnp.int32)
    found = owners[0] * block_rows + local_block[0]
    columns = jnp.where(slot[None, :] < counts[:, None], found, n_row * block_rows).reshape(-1)
    smem = pl.BlockSpec(memory_space=pltpu.SMEM)
    hbm = pl.BlockSpec(memory_space=pl.ANY)
    bf16 = jnp.bfloat16
    dma = pltpu.SemaphoreType.DMA
    return pl.pallas_call(
        functools.partial(kernel, n_row, n_col),
        out_shape=jax.ShapeDtypeStruct(right_sides.shape, bf16),
        in_specs=[smem, hbm, hbm, hbm],
        out_specs=pl.BlockSpec(memory_space=pltpu.VMEM),
        scratch_shapes=[
            pltpu.VMEM((n_row * block_rows + 1, size, width), bf16),
            pltpu.VMEM((block_rows, per_group, size, size), bf16),
            pltpu.VMEM((share, size, width), bf16),
            pltpu.VMEM((share, size, size), bf16),
            pltpu.VMEM((share, size, width), jnp.float32),
            pltpu.VMEM((n_col - 1, share, size, width), bf16),
            pltpu.VMEM((n_col - 1, share, size, width), bf16),
            dma((3,)),
            dma((8, n_row)),
            dma((4 + n_col - 1,)),
            dma((n_col - 1, n_row)),
            dma((n_col - 1,)),
            dma((n_col - 1,)),
            dma((n_col - 1,)),
            dma((n_col - 1,)),
            pltpu.SemaphoreType.REGULAR((4 + n_col - 1,)),
        ],
        compiler_params=pltpu.CompilerParams(
            collective_id=0, has_side_effects=True, vmem_limit_bytes=60 * 1024 * 1024
        ),
    )(
        columns,
        right_sides,
        inverse_diag,
        off_blocks.reshape(off_blocks.shape[1:]),
    )


def solution(mesh):
    in_specs = (
        P("row", None, None),
        P("row", None, None),
        P("col", "row", None, None, None),
        P("col", "row", None),
        P("col", "row", None),
        P("row"),
    )
    body = functools.partial(shards, mesh.shape["row"], mesh.shape["col"])
    return jax.shard_map(
        body, mesh=mesh, in_specs=in_specs, out_specs=P("row", None, None), check_vma=False
    )
```

```python
import functools
import heapq

import jax
import jax.numpy as jnp
from jax import lax
from jax.experimental import pallas as pl
from jax.experimental.pallas import tpu as pltpu
from jax.sharding import PartitionSpec as P

ITERS = 4
MESH = pl.DeviceIdType.MESH
TO_X, TO_Y, TO_UP, TO_DOWN, TO_COL = range(5)
FOUR = (3, 3, 1, 1)
EIGHT = (1,) * 8
EDGE = ("zxy", "zyx", "zxy", "xzy", "yxz", "yzx", "zyx", "xzy")
INNER = ("zyx", "zxy", "zyx", "yzx", "xzy", "zxy", "zyx", "yxz")
ORDERS = ("zxy", "zyx", "xyz", "yxz", "xzy", "yzx")
DEPTH_WEIGHT, DISTANCE_WEIGHT = 0.73, 0.08
PLANE_WEIGHT = dict(zip(ORDERS, (0.62, -0.3, -0.43, -0.82, 0.14, 0.07)))
LINE_WEIGHT = dict(zip(ORDERS, (-1.84, -0.38, 0.41, -1.4, -1.52, -2.03)))
PIECE_TIME, LATENCY, AHEAD = 0.72, 2.4, 1.2


def targets(order, n_z, z, src_z, flip_y, flip_x):
    moved = {"x": flip_x, "y": flip_y, "z": src_z != z}
    found = []
    for place, axis in enumerate(order):
        if any(moved[later] for later in order[place + 1 :]):
            continue
        if axis == "z":
            if src_z <= z < n_z - 1:
                found.append(TO_UP)
            if src_z >= z > 0:
                found.append(TO_DOWN)
        elif not moved[axis]:
            found.append(TO_X if axis == "x" else TO_Y)
    return found


def beyond(z, src_z, flip_y, flip_x, to):
    return {
        TO_X: (z, src_z, flip_y, 1 - flip_x),
        TO_Y: (z, src_z, 1 - flip_y, flip_x),
        TO_UP: (z + 1, src_z, flip_y, flip_x),
        TO_DOWN: (z - 1, src_z, flip_y, flip_x),
    }[to]


@functools.lru_cache(None)
def depth(order, n_z, *where):
    ways = targets(order, n_z, *where)
    return max((1 + depth(order, n_z, *beyond(*where, to)) for to in ways), default=0)


def planned(n_z):
    orders = [EDGE if z in (0, n_z - 1) else INNER for z in range(n_z)]
    events, queued, busy = [], {}, {}
    log = [[] for _ in range(n_z)]
    count = 0
    for z in range(n_z):
        for piece in range(len(EIGHT)):
            events.append((0.0, count, None, piece, (z, z, 0, 0)))
            count += 1
    heapq.heapify(events)
    while events:
        now, touched = events[0][0], set()
        while events and events[0][0] <= now + 1e-9:
            _, _, link, piece, where = heapq.heappop(events)
            if link is not None:
                busy[link] = False
                touched.add(link)
                continue
            z, src_z, flip_y, flip_x = where
            if where != (z, z, 0, 0):
                log[z].append((now, 0, count, (piece, src_z, flip_y, flip_x)))
            order = orders[src_z][piece]
            for to in targets(order, n_z, *where):
                weight = PLANE_WEIGHT if to in (TO_X, TO_Y) else LINE_WEIGHT
                rank = (
                    weight[order]
                    + DISTANCE_WEIGHT * abs(src_z - z)
                    - DEPTH_WEIGHT * depth(order, n_z, *beyond(*where, to))
                )
                heapq.heappush(queued.setdefault((z, to), []), (rank, now, count, piece, where))
                touched.add((z, to))
                count += 1
        for link in sorted(touched):
            if busy.get(link) or not queued.get(link):
                continue
            _, known, _, piece, where = heapq.heappop(queued[link])
            z, to = link
            busy[link] = True
            log[z].append((max(known, now - AHEAD), 1, count, (piece, *where[1:], to)))
            heapq.heappush(events, (now + PIECE_TIME, count + 1, link, None, None))
            heapq.heappush(
                events, (now + PIECE_TIME + LATENCY, count + 2, None, piece, beyond(*where, to))
            )
            count += 3
    return [[entry[3] for entry in sorted(one)] for one in log]


def kernel(
    n_row,
    n_col,
    columns,
    rhs_hbm,
    inv_hbm,
    off_hbm,
    out,
    xg,
    off,
    rhs,
    inv,
    mine,
    outgoing,
    incoming,
    load_sem,
    recv_sem,
    send_sem,
    col_sem,
    part_send,
    part_recv,
    out_send,
    out_recv,
    ready,
):
    row, col = lax.axis_index("row"), lax.axis_index("col")
    block_rows, per_group, size = off.shape[0], off.shape[1], off.shape[2]
    share = block_rows // n_col
    by_blocks = share % 8 == 0
    short = n_row // 4 <= 4
    eighths_of = EIGHT if short else FOUR
    n_z = n_row // 4
    x, y, z = row % 2, (row // 2) % 2, row // 4
    has_up, has_down = z < n_z - 1, z > 0
    target_row = {
        TO_X: row + 1 - 2 * x,
        TO_Y: row + 2 - 4 * y,
        TO_UP: row + 4,
        TO_DOWN: row - 4,
    }
    back = {TO_X: TO_X, TO_Y: TO_Y, TO_UP: TO_DOWN, TO_DOWN: TO_UP}
    others = [(col + step) % n_col for step in range(1, n_col)]

    loads = []
    first = col * share
    for number, (src, dst) in enumerate(
        (
            (rhs_hbm.at[pl.ds(first, share)], rhs),
            (inv_hbm.at[pl.ds(first, share)], inv),
            (off_hbm, off),
        )
    ):
        copy = pltpu.make_async_copy(src, dst, load_sem.at[number])
        copy.start()
        loads.append(copy)

    def greet(semaphore_of):
        for to in (TO_X, TO_Y):
            pl.semaphore_signal(
                semaphore_of(back[to]), inc=1, device_id=(target_row[to], col), device_id_type=MESH
            )
        for to, there in ((TO_UP, has_up), (TO_DOWN, has_down)):

            @pl.when(there)
            def _():
                pl.semaphore_signal(
                    semaphore_of(back[to]),
                    inc=1,
                    device_id=(target_row[to], col),
                    device_id_type=MESH,
                )

        for step, other in enumerate(others):
            pl.semaphore_signal(
                semaphore_of(TO_COL + step), inc=1, device_id=(row, other), device_id_type=MESH
            )

    barrier = pltpu.get_barrier_semaphore()
    greet(lambda which: barrier)
    pl.semaphore_wait(
        barrier, 2 + len(others) + has_up.astype(jnp.int32) + has_down.astype(jnp.int32)
    )

    def start_of(of_col, of_row):
        return of_row * block_rows + of_col * share

    def whole_share(of_col, of_row):
        return xg.at[pl.ds(start_of(of_col, of_row), share)]

    def piece_of(piece, src):
        return part_of(src, sum(eighths_of[:piece]), eighths_of[piece])

    def part_of(src, begin, eighths):
        if by_blocks:
            return xg.at[pl.ds(start_of(col, src) + begin * share // 8, eighths * share // 8)]
        rows = size // 8
        return xg.at[pl.ds(start_of(col, src), share), pl.ds(begin * rows, eighths * rows)]

    def eighths_of_share(eighths):
        if by_blocks:
            return xg.at[pl.ds(0, eighths * share // 8)]
        return xg.at[pl.ds(0, eighths * share), pl.ds(0, size // 8)]

    def remote(piece, src, to):
        return pltpu.make_async_remote_copy(
            src_ref=piece_of(piece, src),
            dst_ref=piece_of(piece, src),
            send_sem=send_sem.at[to],
            recv_sem=recv_sem.at[piece, src],
            device_id=(target_row[to], col),
            device_id_type=MESH,
        )

    def send(piece, src, to):
        remote(piece, src, to).start()

    def arrived(piece, src):
        remote(piece, src, TO_X).wait_recv()

    def send_z(piece, src, ways=(TO_UP, TO_DOWN)):
        for to in ways:

            @pl.when(has_up if to == TO_UP else has_down)
            def _():
                send(piece, src, to)

    def share_copy(src, step, begin=0, eighths=8):
        return pltpu.make_async_remote_copy(
            src_ref=part_of(src, begin, eighths),
            dst_ref=part_of(src, begin, eighths),
            send_sem=send_sem.at[TO_COL + step],
            recv_sem=col_sem.at[step, src],
            device_id=(row, others[step]),
            device_id_type=MESH,
        )

    def at(plane, flip_y, flip_x):
        there_y = 1 - y if flip_y else y
        there_x = 1 - x if flip_x else x
        return plane * 4 + there_y * 2 + there_x

    FLIPS = ((0, 0), (0, 1), (1, 0), (1, 1))

    def spread_plane(plane):
        arrived(0, at(plane, 0, 1))
        send(0, at(plane, 0, 1), TO_Y)
        arrived(1, at(plane, 1, 0))
        send(1, at(plane, 1, 0), TO_X)
        arrived(0, at(plane, 1, 0))
        arrived(1, at(plane, 0, 1))
        arrived(0, at(plane, 1, 1))
        arrived(1, at(plane, 1, 1))

    def to_columns(plane, own):
        for flip in FLIPS:
            if own and flip == (0, 0):
                continue
            for step in range(n_col - 1):
                share_copy(at(plane, *flip), step).start()

    def gather():
        send(2, row, TO_X)
        send(3, row, TO_Y)
        send(3, row, TO_X)
        send(2, row, TO_Y)
        for piece in range(4):
            send_z(piece, row)
        send(1, row, TO_X)
        send(0, row, TO_Y)
        send(0, row, TO_X)
        send(1, row, TO_Y)
        for step in range(n_col - 1):
            share_copy(row, step).start()
        arrived(2, at(z, 0, 1))
        send(2, at(z, 0, 1), TO_Y)
        send_z(2, at(z, 0, 1))
        arrived(3, at(z, 1, 0))
        send(3, at(z, 1, 0), TO_X)
        send_z(3, at(z, 1, 0))
        for piece, flips in ((2, ((1, 0), (1, 1))), (3, ((0, 1), (1, 1)))):
            for flip in flips:
                arrived(piece, at(z, *flip))
                send_z(piece, at(z, *flip))

        for distance in range(1, n_z + 1):
            for sign, onward in ((-1, TO_UP), (1, TO_DOWN)):
                plane = z + sign * distance
                there = plane >= 0 if sign < 0 else plane < n_z

                if distance < n_z:

                    @pl.when(there)
                    def _():
                        for piece in (0, 1):
                            src = at(plane, 0, 0)
                            arrived(piece, src)
                            send_z(piece, src, (onward,))
                            for to in (TO_X, TO_Y) if piece == 1 else (TO_Y, TO_X):
                                send(piece, src, to)
                        for piece in (2, 3):
                            for flip in FLIPS:
                                arrived(piece, at(plane, *flip))
                                send_z(piece, at(plane, *flip), (onward,))

                if distance == 1:
                    if sign < 0:
                        spread_plane(z)
                        to_columns(z, True)
                    continue
                before = z + sign * (distance - 1)
                was_there = before >= 0 if sign < 0 else before < n_z

                @pl.when(was_there)
                def _():
                    spread_plane(before)
                    to_columns(before, False)

    def gather_by_plan(my_z, plan):
        have = {}
        sent_to = dict.fromkeys((TO_X, TO_Y, TO_UP, TO_DOWN), 0)
        for step in range(n_col - 1):
            share_copy(row, step).start()
        for piece, src_z, flip_y, flip_x, *to in plan:
            src = at(src_z, flip_y, flip_x)
            if to:
                send(piece, src, to[0])
                sent_to[to[0]] += 1
                continue
            arrived(piece, src)
            half = (src_z, flip_y, flip_x, piece // 4)
            have[half] = have.get(half, 0) + 1
            if have[half] == 4:
                for step in range(n_col - 1):
                    share_copy(src, step, piece // 4 * 4, 4).start()
        for to, number in sent_to.items():
            if number:
                sent(to, number)

    def finish_columns():
        for step in range(n_col - 1):
            sender = others[n_col - 2 - step]
            for src in range(n_row):
                pltpu.make_async_remote_copy(
                    src_ref=whole_share(sender, src),
                    dst_ref=whole_share(sender, src),
                    send_sem=send_sem.at[TO_COL + step],
                    recv_sem=col_sem.at[step, src],
                    device_id=(row, others[step]),
                    device_id_type=MESH,
                ).wait_recv()
            sent(TO_COL + step, 8 * n_row)

    def sent(to, eighths):
        part = eighths_of_share(eighths)
        pltpu.make_async_copy(part, part, send_sem.at[to]).wait()

    def finish_sends():
        for to in (TO_X, TO_Y):
            sent(to, n_z * 9 + 3)
        for to, there, ahead in ((TO_UP, has_up, z), (TO_DOWN, has_down, n_z - 1 - z)):
            for earlier in range(n_z - 1):

                @pl.when(jnp.logical_and(there, earlier <= ahead))
                def _():
                    sent(to, 14)


    def product(i):
        left = jnp.concatenate([off[i, k] for k in range(per_group)], axis=1)
        right = jnp.concatenate(
            [xg[columns[k, i]] for k in range(per_group)], axis=0
        )
        return jnp.dot(left, right, preferred_element_type=jnp.float32).astype(jnp.bfloat16)

    def part_copy(step):
        return pltpu.make_async_remote_copy(
            src_ref=outgoing.at[step],
            dst_ref=incoming.at[step],
            send_sem=part_send.at[step],
            recv_sem=part_recv.at[step],
            device_id=(row, others[step]),
            device_id_type=MESH,
        )

    own_start = start_of(col, row)

    xg[n_col * n_row * share] = jnp.zeros(xg.shape[1:], xg.dtype)
    loads[0].wait()
    loads[1].wait()

    for j in range(share):
        solved = jnp.dot(inv[j], rhs[j], preferred_element_type=jnp.float32)
        xg[own_start + j] = solved.astype(jnp.bfloat16)
    loads[2].wait()

    def iterate(turn, carry):
        @pl.when(turn > 0)
        def _():
            for to in (TO_X, TO_Y):
                pl.semaphore_wait(ready.at[to], 1)
            for to, there in ((TO_UP, has_up), (TO_DOWN, has_down)):

                @pl.when(there)
                def _():
                    pl.semaphore_wait(ready.at[to], 1)

            for step in range(n_col - 1):
                pl.semaphore_wait(ready.at[TO_COL + step], 1)

        if short:
            for my_z, plan in enumerate(planned(n_z)):
                pl.when(z == my_z)(functools.partial(gather_by_plan, my_z, plan))
        else:
            gather()
            finish_sends()
        finish_columns()
        for step in range(n_col - 1):
            for j in range(share):
                outgoing[step, j] = product(others[step] * share + j)
            part_copy(step).start()
        for j in range(share):
            mine[j] = product(col * share + j).astype(jnp.float32)

        @pl.when(turn < ITERS - 2)
        def _():
            greet(lambda which: ready.at[which])

        for step in range(n_col - 1):
            part_copy(step).wait()
        for j in range(share):
            total = mine[j]
            for step in range(n_col - 1):
                total = total + incoming[step, j].astype(jnp.float32)
            corrected = (rhs[j].astype(jnp.float32) - total).astype(jnp.bfloat16)
            solved = jnp.dot(inv[j], corrected, preferred_element_type=jnp.float32)
            xg[own_start + j] = solved.astype(jnp.bfloat16)
        return carry

    lax.fori_loop(0, ITERS - 1, iterate, 0)

    def out_copy(step):
        part = out.at[pl.ds(col * share, share)]
        return pltpu.make_async_remote_copy(
            src_ref=whole_share(col, row),
            dst_ref=part,
            send_sem=out_send.at[step],
            recv_sem=out_recv.at[step],
            device_id=(row, others[step]),
            device_id_type=MESH,
        )

    for step in range(n_col - 1):
        out_copy(step).start()
    out[pl.ds(col * share, share)] = xg[pl.ds(own_start, share)]
    for step in range(n_col - 1):
        out_copy(step).wait()


def shards(n_row, n_col, right_sides, inverse_diag, off_blocks, owners, local_block, counts):
    block_rows, size, width = right_sides.shape
    per_group = owners.shape[2]
    share = block_rows // n_col
    slot = lax.axis_index("col") + n_col * lax.broadcasted_iota(
        jnp.int32, (per_group, block_rows), 0
    )
    found = owners[0].T * block_rows + local_block[0].T
    columns = jnp.where(slot < counts[None, :], found, n_row * block_rows)
    smem = pl.BlockSpec(memory_space=pltpu.SMEM)
    hbm = pl.BlockSpec(memory_space=pl.ANY)
    bf16 = jnp.bfloat16
    dma = pltpu.SemaphoreType.DMA
    return pl.pallas_call(
        functools.partial(kernel, n_row, n_col),
        out_shape=jax.ShapeDtypeStruct(right_sides.shape, bf16),
        in_specs=[smem, hbm, hbm, hbm],
        out_specs=pl.BlockSpec(memory_space=pltpu.VMEM),
        scratch_shapes=[
            pltpu.VMEM((n_row * block_rows + 1, size, width), bf16),
            pltpu.VMEM((block_rows, per_group, size, size), bf16),
            pltpu.VMEM((share, size, width), bf16),
            pltpu.VMEM((share, size, size), bf16),
            pltpu.VMEM((share, size, width), jnp.float32),
            pltpu.VMEM((n_col - 1, share, size, width), bf16),
            pltpu.VMEM((n_col - 1, share, size, width), bf16),
            dma((3,)),
            dma((8, n_row)),
            dma((4 + n_col - 1,)),
            dma((n_col - 1, n_row)),
            dma((n_col - 1,)),
            dma((n_col - 1,)),
            dma((n_col - 1,)),
            dma((n_col - 1,)),
            pltpu.SemaphoreType.REGULAR((4 + n_col - 1,)),
        ],
        compiler_params=pltpu.CompilerParams(
            collective_id=0, has_side_effects=True, vmem_limit_bytes=60 * 1024 * 1024
        ),
    )(
        columns,
        right_sides,
        inverse_diag,
        off_blocks.reshape(off_blocks.shape[1:]),
    )


def solution(mesh):
    in_specs = (
        P("row", None, None),
        P("row", None, None),
        P("col", "row", None, None, None),
        P("col", "row", None),
        P("col", "row", None),
        P("row"),
    )
    body = functools.partial(shards, mesh.shape["row"], mesh.shape["col"])
    return jax.shard_map(
        body, mesh=mesh, in_specs=in_specs, out_specs=P("row", None, None), check_vma=False
    )
```
